32 devices in a mesh: row: 4 (over y, x), col: 8 (over z, core).
Axes of the slice: x: 2, y: 2, z: 4, core: 2. Of those that a mesh axis runs over, the one named last changes fastest.
Arguments:
- features: float32 [8, 1536, 256], P('col', 'row'), may hold values from -1000 to 1000
- tiles: bfloat16 [8, 4, 8, 9, 128, 128], P('col', 'row'), may hold values from -0.1875 to 0.1875
- tile_ids: int32 [8, 4, 8, 9], P('col', 'row'), may hold values from 0 to 35
- tile_counts: int32 [8, 4, 8], P('col', 'row'), may hold values from 1 to 9, as said below
Outputs:
- propagated: float32 [8, 1536, 256], P('col', 'row')
- residual_norms: float32 [3], replicated
The draws below stay inside these ranges and needn't reach their ends.
Inputs may be any that keep to these rules, and one draw needn't show every extreme that they name: `tile_ids`: each id is a row tile times 3 plus a column tile; ids may repeat within a list. `tile_counts`: slots at or after the count hold values to be ignored; in every draw some device has 9 live slots for some source block.
All inputs are finite; a program needn't handle non-finite values.
Results may differ from the reference program's by a relative error of at most 0.014.
Values may be sent and summed in bfloat16 or wider, within the bound.
A program may use at most 64 MiB of HBM per device.

```python
import jax
import jax.numpy as jnp
from jax import lax

F = 256
TILE = 128
ITERS = 3
NODE_DEV = 384
COARSE = 8
GROUPS_R = 4
FINE = 1536
ROW_TILES = 12
COL_TILES = 3
SLOTS = 9


def draw_features(key, part):
    keys = jax.random.split(jax.random.fold_in(key, 11), 3)
    row_scale = jnp.exp(jax.random.uniform(keys[1], (COARSE, FINE, 1), jnp.float32, -1.2, 1.2))
    col_scale = jnp.exp(jax.random.uniform(keys[2], (1, 1, F), jnp.float32, -1.2, 1.2))
    inner = jnp.arange(FINE, dtype=jnp.float32).reshape(1, FINE, 1) / FINE
    outer = jnp.arange(COARSE, dtype=jnp.float32).reshape(COARSE, 1, 1) / COARSE
    base = jnp.clip(jax.random.normal(keys[0], (COARSE, FINE, F), jnp.float32), -6.0, 6.0)
    rising = (1.0 + 5.0 * inner) * (0.7 + 0.6 * outer)
    return (base * row_scale * col_scale * rising).astype(jnp.float32)


def draw_tile_counts(key, part):
    keys = jax.random.split(jax.random.fold_in(key, 7), 3)
    limits = jax.random.randint(keys[0], (COARSE, GROUPS_R, 1), max(SLOTS // 3, 1), SLOTS + 1)
    counts = jax.random.randint(keys[1], (COARSE, GROUPS_R, COARSE), 1, limits + 1)
    chosen = jax.random.randint(keys[2], (), 0, COARSE * GROUPS_R * COARSE)
    position = jnp.arange(COARSE * GROUPS_R * COARSE, dtype=jnp.int32).reshape(COARSE, GROUPS_R, COARSE)
    return jnp.where(position == chosen, SLOTS, counts).astype(jnp.int32)


def set_ends(values, key, smallest, largest):
    longest = values.shape.index(max(values.shape))
    spots = []
    for shift in (0, 1):
        where = [jax.random.randint(jax.random.fold_in(key, axis), (), 0, length) for axis, length in enumerate(values.shape)]
        where[longest] = (where[longest] + shift) % values.shape[longest]
        spots.append(tuple(where))
    return values.at[spots[0]].set(smallest).at[spots[1]].set(largest)


def levels(key, dims, cuts, low, top_value):
    loudness, own = 1.0, jax.random.fold_in(key, 6)
    for dim, blocks in cuts:
        heights = jnp.exp(jax.random.uniform(jax.random.fold_in(own, dim), (blocks,), jnp.float32, low / len(cuts), top_value / len(cuts)))
        loudness = loudness * jnp.repeat(heights, dims[dim] // blocks).reshape([-1 if axis == dim else 1 for axis in range(len(dims))])
    return loudness


def scatter_about(own_key, shape, spread, limit, cuts=(), kind=jnp.bfloat16):
    drawn = spread * jax.random.normal(own_key, shape, jnp.float32)
    if cuts:
        drawn = drawn * levels(own_key, shape, cuts, -0.22, 0.18)
    return jnp.clip(drawn, -limit, limit).astype(kind)


def setup_inputs(seed: int = 0) -> dict:
    arg_keys = jax.random.split(jax.random.key(seed), 5)
    features = draw_features(jax.random.fold_in(arg_keys[4], 71), 0)
    tiles = scatter_about(arg_keys[1], (COARSE, GROUPS_R, COARSE, SLOTS, TILE, TILE), (9 * TILE * COARSE // (2 * GROUPS_R)) ** -0.5, 0.1875, ((0, 8), (1, 4)))
    tile_ids = set_ends(jax.random.randint(arg_keys[2], (COARSE, GROUPS_R, COARSE, SLOTS), 0, ROW_TILES * COL_TILES), jax.random.fold_in(arg_keys[2], 1), 0, (ROW_TILES * COL_TILES) - 1).astype(jnp.int32)
    tile_counts = draw_tile_counts(jax.random.fold_in(arg_keys[4], 71), 0)
    return {"features": features, "tiles": tiles, "tile_ids": tile_ids, "tile_counts": tile_counts}


def source_term(running, source_block, matrices, slot_ids, live_count):
    tile_size = matrices.shape[-1]
    slot_count = slot_ids.shape[0]
    row_tiles = running.shape[0]
    columns = source_block.shape[-1]
    col_tiles = source_block.shape[0] // tile_size
    pieces = source_block.reshape(col_tiles, tile_size, columns)
    picked = jnp.take(pieces, slot_ids % col_tiles, axis=0)
    products = jnp.einsum('sij,sjf->sif', matrices.astype(jnp.float32), picked.astype(jnp.float32), precision=lax.Precision.HIGHEST)
    in_use = lax.iota(jnp.int32, slot_count) < live_count
    placement = ((slot_ids // col_tiles)[None, :] == lax.iota(jnp.int32, row_tiles)[:, None]) & in_use[None, :]
    return running + jnp.einsum('rs,sif->rif', placement.astype(jnp.float32), products, precision=lax.Precision.HIGHEST)

def device_partial(dev_tiles, dev_ids, dev_counts, sources):
    zeroed = jnp.zeros((ROW_TILES, TILE, F), jnp.float32)

    def sweep(running, source):
        result = source_term(running, sources[source], dev_tiles[source], dev_ids[source], dev_counts[source])
        return (result, None)
    running, _ = lax.scan(sweep, zeroed, jnp.arange(COARSE, dtype=jnp.int32))
    return running

def reference(features, tiles, tile_ids, tile_counts):
    current = features
    squares = []
    for iteration in range(ITERS):
        rounded = current.astype(jnp.bfloat16).reshape(COARSE, GROUPS_R, NODE_DEV, F)

        def per_coarse(coarse):

            def per_group(running, group):
                sources = rounded[:, group]
                partial_value = device_partial(tiles[coarse, group], tile_ids[coarse, group], tile_counts[coarse, group], sources)
                return (running + partial_value, None)
            start_sum = jnp.zeros((ROW_TILES, TILE, F), jnp.float32)
            running, _ = lax.scan(per_group, start_sum, jnp.arange(GROUPS_R, dtype=jnp.int32))
            return running.reshape(FINE, F)
        product = lax.map(per_coarse, jnp.arange(COARSE, dtype=jnp.int32))
        updated = 0.9 * product + 0.1 * features
        squares.append(jnp.sum((updated - current) ** 2))
        current = updated
    residual_norms = jnp.sqrt(jnp.stack(squares) / (COARSE * FINE * F))
    return (current, residual_norms)
```

```python
import functools

import jax
import jax.numpy as jnp
from jax import lax
from jax.experimental import pallas as pl
from jax.experimental.pallas import tpu as pltpu
from jax.sharding import PartitionSpec as P

ITERS = 3
ALPHA = 0.1
CHUNKS = 2
MESH = pl.DeviceIdType.MESH


def kernel(
    nrow, ncol, prev_ref, last_ref, feat_ref, tiles_ref, out_ref, norm_ref,
    dense, buf0, buf1, gathered, acc, current, stage, landed, squares, sq_row, sq_col,
    tile_sem, ag_send, ag_recv, d2d_send, rs_send, rs_recv, sq_send_row, sq_recv_row, sq_send_col, sq_recv_col,
):
    nz = ncol // 2
    nodes, feats = feat_ref.shape
    slots = tiles_ref.shape[1]
    tile = tiles_ref.shape[-1]
    width = feats // CHUNKS
    row_tiles = nrow * nodes // tile
    col_tiles = nodes // tile
    r = lax.axis_index("row")
    c = lax.axis_index("col")
    z = c // 2
    core = c % 2
    sibling = z * 2 + 1 - core
    bufs = (buf0, buf1)

    def tile_copy(q, slot):
        return pltpu.make_async_copy(
            tiles_ref.at[pl.ds(2 * q, 2)], bufs[slot].at[:, pl.ds(0, slots)], tile_sem.at[slot]
        )

    for slot in range(2):
        tile_copy(slot, slot).start()

    barrier = pltpu.get_barrier_semaphore()
    for k in range(1, ncol):
        pl.semaphore_signal(barrier, inc=1, device_id={"col": (c + k) % ncol}, device_id_type=MESH)
    for k in range(1, nrow):
        pl.semaphore_signal(barrier, inc=1, device_id={"row": (r + k) % nrow}, device_id_type=MESH)
    for ch in range(CHUNKS):
        cols = slice(ch * width, (ch + 1) * width)
        gathered[0, ch, c] = feat_ref[:, cols].astype(jnp.bfloat16)
    pl.semaphore_wait(barrier, ncol - 1 + nrow - 1)

    def peer(k):
        if nz == 4:
            return (z, z + 1 - 2 * (z % 2), (z + 2) % 4, 3 - z)[k]
        return (z + k) % nz

    def block_copy(t, ch, source, target, send_sem):
        par = t % 2
        ref = gathered.at[par, ch, source]
        return pltpu.make_async_remote_copy(
            src_ref=ref, dst_ref=ref, send_sem=send_sem, recv_sem=ag_recv.at[par, ch, source],
            device_id={"col": target}, device_id_type=MESH,
        )

    far = [nz == 4 and k == 3 for k in range(nz)]

    def direct(k, act):
        if far[k]:
            pl.when((z == 1) | (z == 2))(act)
        else:
            act()

    send_order = [2, 1, 3] if nz == 4 else list(range(1, nz))

    def gather_send(t, ch):
        for k in send_order:
            def go(k=k):
                copy = block_copy(t, ch, c, peer(k) * 2 + core, ag_send.at[ch, k])
                if t > 0:
                    copy.wait_send()
                copy.start()
            direct(k, go)
        copy = block_copy(t, ch, c, sibling, d2d_send.at[ch, 0])
        if t > 0:
            copy.wait_send()
        copy.start()

    def gather_drain(ch):
        for k in send_order:
            def go(k=k):
                block_copy(0, ch, c, peer(k) * 2 + core, ag_send.at[ch, k]).wait_send()
            direct(k, go)
        for k in range(nz):
            block_copy(0, ch, c, sibling, d2d_send.at[ch, k]).wait_send()
        if nz == 4:
            @pl.when((z == 1) | (z == 2))
            def _():
                block_copy(0, ch, c, sibling, ag_send.at[ch, 0]).wait_send()

    def receive(t, ch, k):
        source = peer(k) * 2 + core
        block_copy(t, ch, source, sibling, d2d_send.at[ch, k]).wait_recv()
        if nz == 4 and k == 2:
            @pl.when((z == 1) | (z == 2))
            def _():
                copy = block_copy(t, ch, source, 6 * (z - 1) + core, ag_send.at[ch, 0])
                if t > 0:
                    copy.wait_send()
                copy.start()
        copy = block_copy(t, ch, source, sibling, d2d_send.at[ch, k])
        if t > 0:
            copy.wait_send()
        copy.start()

    def share_copy(t, ch, k):
        par = t % 2
        return pltpu.make_async_remote_copy(
            src_ref=stage.at[ch, k - 1], dst_ref=landed.at[par, ch, r],
            send_sem=rs_send.at[ch, k - 1], recv_sem=rs_recv.at[par, ch, r],
            device_id={"row": (r + k) % nrow}, device_id_type=MESH,
        )

    def product(t, ch, k):
        q = peer(k)
        par = t % 2
        other = q * 2 + 1 - core
        block_copy(t, ch, other, sibling, d2d_send.at[ch, 0]).wait_recv()
        source = gathered[par, ch, pl.ds(2 * q, 2)].reshape(2 * nodes, width)

        def part(j):
            return jnp.dot(dense[q, pl.ds(j * nodes, nodes)], source, preferred_element_type=jnp.float32)

        if k < nz - 1:
            def one(j, carry):
                rows = pl.ds(j * nodes, nodes)
                acc[ch, rows] = part(j) if k == 0 else acc[ch, rows] + part(j)
                return carry
            lax.fori_loop(0, nrow, one, 0)
            return
        for k2 in list(range(1, nrow)) + [0]:
            j = (r + k2) % nrow
            rows = pl.ds(j * nodes, nodes)
            total = acc[ch, rows] + part(j)
            if k2 == 0:
                acc[ch, rows] = total
                continue
            if t > 0:
                share_copy(t, ch, k2).wait_send()
            stage[ch, k2 - 1] = total.astype(jnp.bfloat16)
            share_copy(t, ch, k2).start()

    def update(t, ch):
        par = t % 2
        cols = slice(ch * width, (ch + 1) * width)
        summed = acc[ch, pl.ds(r * nodes, nodes)]
        for k in range(1, nrow):
            j = (r + k) % nrow
            pltpu.make_async_remote_copy(
                src_ref=stage.at[ch, 0], dst_ref=landed.at[par, ch, j], send_sem=rs_send.at[ch, 0],
                recv_sem=rs_recv.at[par, ch, j], device_id={"row": j}, device_id_type=MESH,
            ).wait_recv()
            summed = summed + landed[par, ch, j].astype(jnp.float32)
        teleport = feat_ref[:, cols]
        updated = (1.0 - ALPHA) * summed + ALPHA * teleport
        before = teleport if t == 0 else current[:, cols]
        if t < ITERS - 1:
            gathered[(t + 1) % 2, ch, c] = updated.astype(jnp.bfloat16)
            gather_send(t + 1, ch)
            current[:, cols] = updated
        else:
            out_ref[:, cols] = updated
        change = jnp.sum((updated - before) ** 2, axis=0, keepdims=True)
        squares[t : t + 1] = change if ch == 0 else squares[t : t + 1] + change

    for ch in range(CHUNKS):
        gather_send(0, ch)

    zero = jnp.zeros((tile, tile), jnp.bfloat16)
    for slot in range(2):
        for half in range(2):
            bufs[slot][half, slots] = zero

    def build(step, carry):
        for slot in range(2):
            q = step * 2 + slot
            buf = bufs[slot]
            tile_copy(q, slot).wait()
            for half in range(2):
                s = 2 * q + half
                for k in range(1, slots):
                    buf[half, k] = buf[half, k] + buf[half, prev_ref[s, k]]
                for i in range(row_tiles):
                    for j in range(col_tiles):
                        at = half * nodes + j * tile
                        dense[q, i * tile : (i + 1) * tile, at : at + tile] = buf[half, last_ref[s, i * col_tiles + j]]

            @pl.when(q + 2 < nz)
            def _():
                tile_copy(q + 2, slot).start()
        return carry

    squares[...] = jnp.zeros_like(squares)
    lax.fori_loop(0, nz // 2, build, 0)

    pending = None
    for t in range(ITERS):
        for ch in range(CHUNKS):
            for k in range(1, nz):
                receive(t, ch, k)
                if k == nz - 1 and pending is not None:
                    update(*pending)
                product(t, ch, k - 1)
            product(t, ch, nz - 1)
            pending = (t, ch)
    update(*pending)

    def sq_copy(axis, size, me, k, buffer, send, recv):
        return pltpu.make_async_remote_copy(
            src_ref=buffer.at[me], dst_ref=buffer.at[me], send_sem=send.at[k], recv_sem=recv.at[me],
            device_id={axis: (me + k) % size}, device_id_type=MESH,
        )

    total = squares[...]
    for axis, size, me, buffer, send, recv in (
        ("row", nrow, r, sq_row, sq_send_row, sq_recv_row),
        ("col", ncol, c, sq_col, sq_send_col, sq_recv_col),
    ):
        buffer[me] = total
        for k in range(1, size):
            sq_copy(axis, size, me, k, buffer, send, recv).start()
        for k in range(1, size):
            j = (me + k) % size
            pltpu.make_async_remote_copy(
                src_ref=buffer.at[me], dst_ref=buffer.at[j], send_sem=send.at[k], recv_sem=recv.at[j],
                device_id={axis: j}, device_id_type=MESH,
            ).wait_recv()
        total = buffer[0]
        for j in range(1, size):
            total = total + buffer[j]
        for k in range(1, size):
            sq_copy(axis, size, me, k, buffer, send, recv).wait_send()
    count = nrow * ncol * nodes * feats
    norms = jnp.sqrt(jnp.sum(total, axis=1, keepdims=True) / count)
    norm_ref[...] = jnp.broadcast_to(norms, norm_ref.shape)

    for ch in range(CHUNKS):
        gather_drain(ch)
        for k in range(1, nrow):
            share_copy(0, ch, k).wait_send()


def local(nrow, ncol, features, tiles, tile_ids, tile_counts):
    teleport = features[0]
    my_tiles = tiles[0, 0]
    my_ids = tile_ids[0, 0]
    my_counts = tile_counts[0, 0]
    nodes, feats = teleport.shape
    sources, slots, tile, _ = my_tiles.shape
    nz = ncol // 2
    width = feats // CHUNKS
    places = (nrow * nodes // tile) * (nodes // tile)
    slot = lax.iota(jnp.int32, slots)
    live = slot[None, :] < my_counts[:, None]
    same = (my_ids[:, :, None] == my_ids[:, None, :]) & live[:, None, :] & (slot[None, None, :] < slot[None, :, None])
    prev = jnp.max(jnp.where(same, slot[None, None, :], -1), axis=2)
    prev = jnp.where(prev < 0, slots, prev)
    here = (my_ids[:, None, :] == lax.iota(jnp.int32, places)[None, :, None]) & live[:, None, :]
    last = jnp.max(jnp.where(here, slot[None, None, :], -1), axis=2)
    last = jnp.where(last < 0, slots, last)
    bf16, f32 = jnp.bfloat16, jnp.float32
    vmem, smem = pltpu.VMEM, pltpu.SMEM
    dma = pltpu.SemaphoreType.DMA
    out, norms = pl.pallas_call(
        functools.partial(kernel, nrow, ncol),
        out_shape=(jax.ShapeDtypeStruct((nodes, feats), f32), jax.ShapeDtypeStruct((8, 128), f32)),
        in_specs=[
            pl.BlockSpec(memory_space=smem), pl.BlockSpec(memory_space=smem),
            pl.BlockSpec(memory_space=vmem), pl.BlockSpec(memory_space=pl.ANY),
        ],
        out_specs=(pl.BlockSpec(memory_space=vmem), pl.BlockSpec(memory_space=vmem)),
        scratch_shapes=[
            vmem((nz, nrow * nodes, 2 * nodes), bf16),
            vmem((2, slots + 1, tile, tile), bf16),
            vmem((2, slots + 1, tile, tile), bf16),
            vmem((2, CHUNKS, ncol, nodes, width), bf16),
            vmem((CHUNKS, nrow * nodes, width), f32),
            vmem((nodes, feats), f32),
            vmem((CHUNKS, nrow - 1, nodes, width), bf16),
            vmem((2, CHUNKS, nrow, nodes, width), bf16),
            vmem((8, width), f32),
            vmem((nrow, 8, width), f32),
            vmem((ncol, 8, width), f32),
            dma((2,)),
            dma((CHUNKS, nz)),
            dma((2, CHUNKS, ncol)),
            dma((CHUNKS, nz)),
            dma((CHUNKS, nrow - 1)),
            dma((2, CHUNKS, nrow)),
            dma((nrow,)),
            dma((nrow,)),
            dma((ncol,)),
            dma((ncol,)),
        ],
        compiler_params=pltpu.CompilerParams(collective_id=0, has_side_effects=True),
    )(prev, last, teleport, my_tiles)
    return (out[None], norms[:ITERS, 0])


def solution(mesh):
    in_specs = (
        P("col", "row", None),
        P("col", "row", None, None, None, None),
        P("col", "row", None, None),
        P("col", "row", None),
    )
    out_specs = (P("col", "row", None), P())
    body = functools.partial(local, mesh.shape["row"], mesh.shape["col"])
    return jax.shard_map(body, mesh=mesh, in_specs=in_specs, out_specs=out_specs, check_vma=False)
```

```python
import functools

import jax
import jax.numpy as jnp
from jax import lax
from jax.experimental import pallas as pl
from jax.experimental.pallas import tpu as pltpu
from jax.sharding import PartitionSpec as P

ITERS = 3
ALPHA = 0.1
CHUNKS = 2
PIECES = 2
MESH = pl.DeviceIdType.MESH


def kernel(
    nrow, ncol, ids_ref, counts_ref, feat_ref, tiles_ref, out_ref, norm_ref,
    table, lookup, dense, buf0, buf1, gathered, acc, current, stage, landed, squares, sq_row, sq_col,
    table_sem, tile_sem, ag_send, ag_recv, d2d_send, rs_send, rs_recv, sq_send_row, sq_recv_row, sq_send_col, sq_recv_col,
):
    nz = ncol // 2
    nodes, feats = feat_ref.shape
    slots = tiles_ref.shape[1]
    tile = tiles_ref.shape[-1]
    width = feats // CHUNKS
    row_tiles = nrow * nodes // tile
    col_tiles = nodes // tile
    places = row_tiles * col_tiles
    r = lax.axis_index("row")
    c = lax.axis_index("col")
    z = c // 2
    core = c % 2
    sibling = z * 2 + 1 - core
    bufs = (buf0, buf1)

    def tile_copy(q, slot):
        return pltpu.make_async_copy(
            tiles_ref.at[pl.ds(2 * q, 2)], bufs[slot].at[:, pl.ds(0, slots)], tile_sem.at[slot]
        )

    for slot in range(2):
        tile_copy(slot, slot).start()

    barrier = pltpu.get_barrier_semaphore()
    for k in range(1, ncol):
        pl.semaphore_signal(barrier, inc=1, device_id={"col": (c + k) % ncol}, device_id_type=MESH)
    for k in range(1, nrow):
        pl.semaphore_signal(barrier, inc=1, device_id={"row": (r + k) % nrow}, device_id_type=MESH)
    for ch in range(CHUNKS):
        cols = slice(ch * width, (ch + 1) * width)
        gathered[0, ch, c] = feat_ref[:, cols].astype(jnp.bfloat16)
    pl.semaphore_wait(barrier, ncol - 1 + nrow - 1)

    def peer(k):
        if nz == 4:
            return (z, z + 1 - 2 * (z % 2), (z + 2) % 4, 3 - z)[k]
        return (z + k) % nz

    piece = nodes // PIECES

    def block_copy(t, ch, source, target, send_sem, h):
        par = t % 2
        ref = gathered.at[par, ch, source, pl.ds(h * piece, piece)]
        return pltpu.make_async_remote_copy(
            src_ref=ref, dst_ref=ref, send_sem=send_sem, recv_sem=ag_recv.at[par, ch, source, h],
            device_id={"col": target}, device_id_type=MESH,
        )

    far = [nz == 4 and k == 3 for k in range(nz)]

    def direct(k, act):
        if far[k]:
            pl.when((z == 1) | (z == 2))(act)
        else:
            act()

    send_order = [2, 1, 3] if nz == 4 else list(range(1, nz))

    def gather_drain(ch, h):
        for k in send_order:
            def go(k=k):
                block_copy(0, ch, c, peer(k) * 2 + core, ag_send.at[ch, k, h], h).wait_send()
            direct(k, go)
        for k in range(nz):
            block_copy(0, ch, c, sibling, d2d_send.at[ch, k, h], h).wait_send()
        if nz == 4:
            @pl.when((z == 1) | (z == 2))
            def _():
                block_copy(0, ch, c, sibling, ag_send.at[ch, 0, h], h).wait_send()

    def gather_send(t, ch, h):
        if t > 0:
            gather_drain(ch, h)
        for k in send_order:
            def go(k=k):
                block_copy(t, ch, c, peer(k) * 2 + core, ag_send.at[ch, k, h], h).start()
            direct(k, go)
        block_copy(t, ch, c, sibling, d2d_send.at[ch, 0, h], h).start()

    def receive(t, ch, k):
        source = peer(k) * 2 + core
        for h in range(PIECES):
            block_copy(t, ch, source, sibling, d2d_send.at[ch, k, h], h).wait_recv()
            if nz == 4 and k == 2:
                @pl.when((z == 1) | (z == 2))
                def _():
                    block_copy(t, ch, source, 6 * (z - 1) + core, ag_send.at[ch, 0, h], h).start()
            block_copy(t, ch, source, sibling, d2d_send.at[ch, k, h], h).start()

    def share_copy(t, ch, k, h):
        par = t % 2
        span = pl.ds(h * piece, piece)
        return pltpu.make_async_remote_copy(
            src_ref=stage.at[ch, k - 1, span], dst_ref=landed.at[par, ch, r, span],
            send_sem=rs_send.at[ch, k - 1, h], recv_sem=rs_recv.at[par, ch, r, h],
            device_id={"row": (r + k) % nrow}, device_id_type=MESH,
        )

    def product(t, ch, k):
        q = peer(k)
        par = t % 2
        other = q * 2 + 1 - core
        for h in range(PIECES):
            block_copy(t, ch, other, sibling, d2d_send.at[ch, 0, h], h).wait_recv()
        source = gathered[par, ch, pl.ds(2 * q, 2)].reshape(2 * nodes, width)

        def part(rows):
            return jnp.dot(dense[q, rows], source, preferred_element_type=jnp.float32)

        if k < nz - 1:
            def one(j, carry):
                rows = pl.ds(j * nodes, nodes)
                acc[ch, rows] = part(rows) if k == 0 else acc[ch, rows] + part(rows)
                return carry
            lax.fori_loop(0, nrow, one, 0)
            return
        for h in range(PIECES):
            for k2 in range(1, nrow):
                rows = pl.ds((r + k2) % nrow * nodes + h * piece, piece)
                total = acc[ch, rows] + part(rows)
                if t > 0:
                    share_copy(t, ch, k2, h).wait_send()
                stage[ch, k2 - 1, h * piece : (h + 1) * piece] = total.astype(jnp.bfloat16)
                share_copy(t, ch, k2, h).start()
        rows = pl.ds(r * nodes, nodes)
        acc[ch, rows] = acc[ch, rows] + part(rows)

    def update(t, ch):
        par = t % 2
        cols = slice(ch * width, (ch + 1) * width)
        for h in range(PIECES):
            span = slice(h * piece, (h + 1) * piece)
            summed = acc[ch, pl.ds(r * nodes + h * piece, piece)]
            for k in range(1, nrow):
                j = (r + k) % nrow
                spot = landed.at[par, ch, j, pl.ds(h * piece, piece)]
                pltpu.make_async_remote_copy(
                    src_ref=spot, dst_ref=spot, send_sem=rs_send.at[ch, 0, h],
                    recv_sem=rs_recv.at[par, ch, j, h], device_id={"row": j}, device_id_type=MESH,
                ).wait_recv()
                summed = summed + landed[par, ch, j, span].astype(jnp.float32)
            teleport = feat_ref[span, cols]
            updated = (1.0 - ALPHA) * summed + ALPHA * teleport
            before = teleport if t == 0 else current[span, cols]
            if t < ITERS - 1:
                gathered[(t + 1) % 2, ch, c, span] = updated.astype(jnp.bfloat16)
                gather_send(t + 1, ch, h)
                current[span, cols] = updated
            else:
                out_ref[span, cols] = updated
            change = jnp.sum((updated - before) ** 2, axis=0, keepdims=True)
            squares[t : t + 1] = squares[t : t + 1] + change

    squares[...] = jnp.zeros_like(squares)
    for ch in range(CHUNKS):
        for h in range(PIECES):
            gather_send(0, ch, h)

    lane = lax.broadcasted_iota(jnp.int32, (1, table.shape[1]), 1)
    earlier = jnp.where(lane < places, slots, lane - places)

    def find(s, carry):
        ids = [ids_ref[s, k] for k in range(slots)]
        live = counts_ref[s]
        wanted = lane
        for k in range(slots):
            wanted = jnp.where(lane == places + k, ids[k], wanted)
        limit = jnp.minimum(earlier, live)
        found = jnp.full_like(lane, slots)
        for k in range(slots):
            found = jnp.where((wanted == ids[k]) & (limit > k), k, found)
        table[pl.ds(s, 1), :] = found
        return carry

    lax.fori_loop(0, ncol, find, 0)
    to_scalars = pltpu.make_async_copy(table, lookup, table_sem)
    to_scalars.start()
    zero = jnp.zeros((tile, tile), jnp.bfloat16)
    for slot in range(2):
        for half in range(2):
            bufs[slot][half, slots] = zero

    def build(step, carry):
        for slot in range(2):
            q = step * 2 + slot
            buf = bufs[slot]
            tile_copy(q, slot).wait()
            for half in range(2):
                s = 2 * q + half
                for k in range(1, slots):
                    buf[half, k] = buf[half, k] + buf[half, lookup[s, places + k]]
                for i in range(row_tiles):
                    for j in range(col_tiles):
                        at = half * nodes + j * tile
                        dense[q, i * tile : (i + 1) * tile, at : at + tile] = buf[half, lookup[s, i * col_tiles + j]]

            @pl.when(q + 2 < nz)
            def _():
                tile_copy(q + 2, slot).start()
        return carry

    to_scalars.wait()
    lax.fori_loop(0, nz // 2, build, 0)

    pending = None
    for t in range(ITERS):
        for ch in range(CHUNKS):
            for k in range(1, nz):
                if k == nz - 1 and pending is not None:
                    update(*pending)
                receive(t, ch, k)
                product(t, ch, k - 1)
            product(t, ch, nz - 1)
            pending = (t, ch)
    update(*pending)

    def sq_copy(axis, size, me, k, buffer, send, recv):
        return pltpu.make_async_remote_copy(
            src_ref=buffer.at[me], dst_ref=buffer.at[me], send_sem=send.at[k], recv_sem=recv.at[me],
            device_id={axis: (me + k) % size}, device_id_type=MESH,
        )

    total = squares[...]
    for axis, size, me, buffer, send, recv in (
        ("row", nrow, r, sq_row, sq_send_row, sq_recv_row),
        ("col", ncol, c, sq_col, sq_send_col, sq_recv_col),
    ):
        buffer[me] = total
        for k in range(1, size):
            sq_copy(axis, size, me, k, buffer, send, recv).start()
        for k in range(1, size):
            j = (me + k) % size
            pltpu.make_async_remote_copy(
                src_ref=buffer.at[me], dst_ref=buffer.at[j], send_sem=send.at[k], recv_sem=recv.at[j],
                device_id={axis: j}, device_id_type=MESH,
            ).wait_recv()
        total = buffer[0]
        for j in range(1, size):
            total = total + buffer[j]
        for k in range(1, size):
            sq_copy(axis, size, me, k, buffer, send, recv).wait_send()
    count = nrow * ncol * nodes * feats
    norms = jnp.sqrt(jnp.sum(total, axis=1, keepdims=True) / count)
    norm_ref[...] = jnp.broadcast_to(norms, norm_ref.shape)

    for ch in range(CHUNKS):
        for h in range(PIECES):
            gather_drain(ch, h)
            for k in range(1, nrow):
                share_copy(0, ch, k, h).wait_send()


def local(nrow, ncol, features, tiles, tile_ids, tile_counts):
    teleport = features[0]
    my_tiles = tiles[0, 0]
    my_ids = tile_ids[0, 0]
    my_counts = tile_counts[0, 0]
    nodes, feats = teleport.shape
    sources, slots, tile, _ = my_tiles.shape
    nz = ncol // 2
    width = feats // CHUNKS
    places = (nrow * nodes // tile) * (nodes // tile)
    lanes = pl.cdiv(places + slots, 128) * 128
    bf16, f32 = jnp.bfloat16, jnp.float32
    vmem, smem = pltpu.VMEM, pltpu.SMEM
    dma = pltpu.SemaphoreType.DMA
    out, norms = pl.pallas_call(
        functools.partial(kernel, nrow, ncol),
        out_shape=(jax.ShapeDtypeStruct((nodes, feats), f32), jax.ShapeDtypeStruct((8, 128), f32)),
        in_specs=[
            pl.BlockSpec(memory_space=smem), pl.BlockSpec(memory_space=smem),
            pl.BlockSpec(memory_space=vmem), pl.BlockSpec(memory_space=pl.ANY),
        ],
        out_specs=(pl.BlockSpec(memory_space=vmem), pl.BlockSpec(memory_space=vmem)),
        scratch_shapes=[
            vmem((ncol, lanes), jnp.int32),
            smem((ncol, lanes), jnp.int32),
            vmem((nz, nrow * nodes, 2 * nodes), bf16),
            vmem((2, slots + 1, tile, tile), bf16),
            vmem((2, slots + 1, tile, tile), bf16),
            vmem((2, CHUNKS, ncol, nodes, width), bf16),
            vmem((CHUNKS, nrow * nodes, width), f32),
            vmem((nodes, feats), f32),
            vmem((CHUNKS, nrow - 1, nodes, width), bf16),
            vmem((2, CHUNKS, nrow, nodes, width), bf16),
            vmem((8, width), f32),
            vmem((nrow, 8, width), f32),
            vmem((ncol, 8, width), f32),
            dma,
            dma((2,)),
            dma((CHUNKS, nz, PIECES)),
            dma((2, CHUNKS, ncol, PIECES)),
            dma((CHUNKS, nz, PIECES)),
            dma((CHUNKS, nrow - 1, PIECES)),
            dma((2, CHUNKS, nrow, PIECES)),
            dma((nrow,)),
            dma((nrow,)),
            dma((ncol,)),
            dma((ncol,)),
        ],
        compiler_params=pltpu.CompilerParams(collective_id=0, has_side_effects=True),
    )(my_ids, my_counts, teleport, my_tiles)
    return (out[None], norms[:ITERS, 0])


def solution(mesh):
    in_specs = (
        P("col", "row", None),
        P("col", "row", None, None, None, None),
        P("col", "row", None, None),
        P("col", "row", None),
    )
    out_specs = (P("col", "row", None), P())
    body = functools.partial(local, mesh.shape["row"], mesh.shape["col"])
    return jax.shard_map(body, mesh=mesh, in_specs=in_specs, out_specs=out_specs, check_vma=False)
```
